32 devices in a mesh: dp: 4 (over x, core), vocab: 8 (over z, y).
Axes of the slice: x: 2, y: 2, z: 4, core: 2. Of those that a mesh axis runs over, the one named last changes fastest.
Arguments:
- hidden: bfloat16 [128, 8192], P(('dp', 'vocab')), may hold values from -350 to 350
- lm_head: bfloat16 [8192, 128256], P(None, ('dp', 'vocab')), may hold values from -0.0625 to 0.0625
- targets: int32 [128], P(('dp', 'vocab')), may hold values from 0 to 128255
- segment: int32 [128], P(('dp', 'vocab')), may hold values from 0 to 32, as said below
- pad_mask: int32 [128], P(('dp', 'vocab')), may hold values from 0 to 1, as said below
- seq_bench: int32 [33], replicated, may hold values from 0 to 7
Outputs:
- token_nll: float32 [128], P(('dp', 'vocab'))
- bench_total: float32 [8], replicated
- bench_count: float32 [8], replicated
The draws below stay inside these ranges and needn't reach their ends.
Inputs may be any that keep to these rules, and one draw needn't show every extreme that they name: `segment`: sequence numbers never fall along the pack; each aligned block of 4 tokens holds exactly one place inside it where the number rises by one, and the number does not change between one block's last token and the next block's first. `pad_mask`: the last token of each aligned block of 4 tokens is real.
All inputs are finite; a program needn't handle non-finite values.
Results may differ from the reference program's by a relative error of at most 0.0003.
Values may be sent and summed in bfloat16 or wider, within the bound.
A program may use at most 128 MiB of HBM per device.

```python
import math
import jax
import jax.numpy as jnp
import numpy as np
from jax import lax

D = 8192
VOCAB = 128256
TOK_DEV = 4
NBENCH = 8
TOKENS = 128
NSEQ = 33


def draw_hidden(key, part):
    first, second = jax.random.split(key, 2)
    base = jnp.clip(jax.random.normal(first, (TOKENS, D), jnp.float32), -5.0, 5.0)
    scales = 3.0 * jnp.exp(jax.random.uniform(second, (TOKENS,), jnp.float32, -0.3, 0.3))
    return (base * scales[:, None]).astype(jnp.bfloat16)


def draw_segment(key, part):
    blocks = TOKENS // TOK_DEV
    places = jax.random.randint(jax.random.fold_in(key, 11), (blocks,), 1, TOK_DEV)
    local = jnp.arange(TOK_DEV, dtype=jnp.int32)
    rises = (local[None, :] >= places[:, None]).astype(jnp.int32)
    numbers = jnp.arange(blocks, dtype=jnp.int32)[:, None] + rises
    return numbers.reshape(TOKENS).astype(jnp.int32)


def draw_pad_mask(key, part):
    blocks = TOKENS // TOK_DEV
    values = jax.random.randint(jax.random.fold_in(key, 23), (blocks, TOK_DEV), 0, 4)
    real = (values != 0).astype(jnp.int32)
    last = (jnp.arange(TOK_DEV, dtype=jnp.int32) == TOK_DEV - 1).astype(jnp.int32)
    return jnp.maximum(real, last[None, :]).reshape(TOKENS).astype(jnp.int32)


def place_ends(values, rng, smallest, top_value):
    dims = values.shape
    place = [jax.random.randint(jax.random.fold_in(rng, axis), (), 0, dims[axis]) for axis in range(len(dims))]
    values = values.at[tuple(place)].set(smallest)
    longest = dims.index(max(dims))
    place[longest] = (place[longest] + 1) % dims[longest]
    return values.at[tuple(place)].set(top_value)


def block_scale(stream_key, dims, cuts, least, largest):
    def one(axis_at, parts):
        steps = jax.random.uniform(jax.random.fold_in(jax.random.fold_in(stream_key, 6), axis_at), (parts,), jnp.float32, least / len(cuts), largest / len(cuts))
        return jnp.repeat(jnp.exp(steps), dims[axis_at] // parts).reshape((-1,) + (1,) * (len(dims) - axis_at - 1))

    loudness = one(*cuts[0])
    for cut in cuts[1:]:
        loudness = loudness * one(*cut)
    return loudness


def wide_ids(rng, extent, amount, lean):
    loads = [min(1 << octave, amount + 1 - (1 << octave)) * (1 << 20) // math.isqrt((1 << octave) ** lean) + 1 for octave in range((amount + 1).bit_length()) if 1 << octave <= amount]
    width = 1 + sum(loads) // (1 << 30)
    listing = np.cumsum(np.array([max(1, weight // width) for weight in loads]))
    ticket = jax.random.randint(jax.random.fold_in(rng, 1), extent, 0, int(listing[len(loads) - 1]))
    start = jnp.left_shift(1, jnp.searchsorted(jnp.asarray(listing, jnp.int32), ticket, side="right").astype(jnp.int32))
    rank = start - 1 + jax.random.randint(jax.random.fold_in(rng, 4), extent, 0, 1 << 30) % jnp.minimum(start, amount + 1 - start)
    return jax.random.permutation(jax.random.fold_in(rng, 2), amount)[rank].astype(jnp.int32)


def scatter_about(stream_key, dims, scale, most, pieces=(), held_as=jnp.bfloat16):
    drawn = scale * jax.random.normal(stream_key, dims, jnp.float32)
    if pieces:
        drawn = drawn * block_scale(stream_key, dims, pieces, -0.22, 0.18)
    return jnp.clip(drawn, -most, most).astype(held_as)


def setup_inputs(seed: int = 0) -> dict:
    seeds = jax.random.split(jax.random.key(seed), 7)
    return {
        "hidden": draw_hidden(jax.random.fold_in(seeds[6], 71), 0),
        "lm_head": scatter_about(seeds[1], (D, VOCAB), D ** -0.5, 0.0625, ((1, 32),)),
        "targets": place_ends(wide_ids(seeds[2], (TOKENS,), VOCAB, 2), jax.random.fold_in(seeds[2], 3), 0, VOCAB - 1).astype(jnp.int32),
        "segment": draw_segment(jax.random.fold_in(seeds[6], 71), 0),
        "pad_mask": draw_pad_mask(jax.random.fold_in(seeds[6], 71), 0),
        "seq_bench": place_ends(jax.random.randint(seeds[5], (NSEQ,), 0, NBENCH), jax.random.fold_in(seeds[5], 1), 0, NBENCH - 1).astype(jnp.int32),
    }


def reference(hidden, lm_head, targets, segment, pad_mask, seq_bench):
    block = math.gcd(TOKENS, 128)

    def one_block(pair):
        rows, wanted = pair
        logits = jnp.dot(rows, lm_head, preferred_element_type=jnp.float32)
        top = jnp.max(logits, axis=1)
        total = jnp.sum(jnp.exp(logits - top[:, None]), axis=1)
        picked = jnp.take_along_axis(logits, wanted[:, None], axis=1)[:, 0]
        return top + jnp.log(total) - picked

    token_nll = lax.map(one_block, (hidden.reshape(TOKENS // block, block, D), targets.reshape(TOKENS // block, block))).reshape(TOKENS)
    following = jnp.concatenate([segment[1:], jnp.full((1,), -1, jnp.int32)])
    keep = (pad_mask * (segment == following).astype(jnp.int32)).astype(jnp.float32)
    bench = seq_bench[segment]
    bench_hot = (bench[:, None] == jnp.arange(NBENCH, dtype=jnp.int32)[None, :]).astype(jnp.float32)
    bench_total = jnp.sum(bench_hot * (keep * token_nll)[:, None], axis=0)
    bench_count = jnp.sum(bench_hot * keep[:, None], axis=0)
    return token_nll, bench_total, bench_count
```

```python
import functools
import math

import jax
import jax.numpy as jnp
from jax import lax
from jax.experimental import pallas as pl
from jax.experimental.pallas import tpu as pltpu
from jax.sharding import PartitionSpec as P

NBENCH = 8
MESH = pl.DeviceIdType.MESH


def kernel(dims, hid, tgt, seg, pad, kinds, w_hbm, nll_out, total_out, count_out,
           g, wbuf, acc, meta, tgt_v, seg_v, pad_v, kinds_v, mine, sbuf,
           wsem, hsem, isem, zrecv, precv, crecv, zsend, psend, csend,
           mzrecv, mprecv, mcrecv, mzsend, mpsend, mcsend, qsend, qrecv):
    X, Y, Z, V, N, kc, nk, nbuf, td, lead_z, lead_p = dims
    XY, S = X * Y, X * Y * Z
    dp, v = lax.axis_index("dp"), lax.axis_index("vocab")
    me = dp * V + v
    x, core = dp // 2, lax.rem(dp, 2)
    z, y = v // Y, lax.rem(v, Y)
    xy = x * Y + y
    tokens = N * td
    at = (core * S + xy * Z + z) * td

    def zpeer(d):
        zz = lax.rem(z + d, Z)
        return (dp, zz * Y + y), zz

    def ppeer(d):
        t = lax.rem(xy + d, XY)
        return ((t // Y) * 2 + core, z * Y + lax.rem(t, Y)), t

    partner = (x * 2 + 1 - core, v)
    peers = [zpeer(d)[0] for d in range(1, Z)] + [ppeer(d)[0] for d in range(1, XY)] + [partner]

    own = pltpu.make_async_copy(hid, g.at[pl.ds(pl.multiple_of(at, td), td), :], hsem)
    own.start()
    loads = [pltpu.make_async_copy(a, b, isem.at[i]) for i, (a, b) in enumerate(
        ((tgt, tgt_v), (seg, seg_v), (pad, pad_v), (kinds, kinds_v)))]
    for copy in loads:
        copy.start()

    def wcopy(k):
        s = lax.rem(k, nbuf)
        return pltpu.make_async_copy(
            w_hbm.at[:, pl.ds(pl.multiple_of(k * kc, kc), kc)], wbuf.at[s], wsem.at[s])

    for k in range(nbuf):
        wcopy(k).start(priority=1)

    barrier = pltpu.get_barrier_semaphore()
    for peer in peers:
        pl.semaphore_signal(barrier, inc=1, device_id=peer, device_id_type=MESH)

    for copy in loads:
        copy.wait()
    nseq = kinds_v.shape[1]
    last = me == N - 1
    lane = lax.broadcasted_iota(jnp.int32, (1, tokens), 1) - at
    seqs = lax.broadcasted_iota(jnp.int32, (1, nseq), 1)
    wanted = jnp.zeros((1, tokens), jnp.int32)
    kind = jnp.zeros((1, tokens), jnp.int32)
    for j in range(td):
        s = seg_v[:, j:j + 1]
        bench = jnp.sum(jnp.where(seqs == s, kinds_v[...], 0), axis=1, keepdims=True)
        same = s == seg_v[:, j + 1:j + 2] if j + 1 < td else jnp.broadcast_to(jnp.logical_not(last), (1, 1))
        keep = same & (pad_v[:, j:j + 1] != 0)
        wanted = jnp.where(lane == j, tgt_v[:, j:j + 1], wanted)
        kind = jnp.where(lane == j, jnp.where(keep, bench, NBENCH), kind)
    meta[core * S + xy * Z + z] = jnp.concatenate([wanted, kind], axis=0)
    own.wait()
    pl.semaphore_wait(barrier, len(peers))

    def cols(p):
        return pl.ds(pl.multiple_of(p * kc, kc), kc)

    def rows(first, count):
        return pl.ds(pl.multiple_of((core * S + first) * td, td), count * td)

    def remote(src, send, recv, to):
        return pltpu.make_async_remote_copy(src, src, send, recv, device_id=to, device_id_type=MESH)

    def zcopy(p, d):
        ref = g.at[rows(xy * Z + z, 1), cols(p)]
        return remote(ref, zsend.at[p, d], zrecv.at[p, z], zpeer(d)[0])

    def pcopy(p, d):
        ref = g.at[rows(xy * Z, Z), cols(p)]
        return remote(ref, psend.at[p, d], precv.at[p, xy], ppeer(d)[0])

    def ccopy(p):
        ref = g.at[rows(0, S), cols(p)]
        return remote(ref, csend.at[p], crecv.at[p], partner)

    def arrived(ref, sem):
        pltpu.make_async_copy(ref, ref, sem).wait()

    def send_z(p, c):
        for d in range(1, Z):
            zcopy(p, d).start()
        return c

    def from_z(p, c=0):
        for d in range(1, Z):
            zz = zpeer(d)[1]
            arrived(g.at[rows(xy * Z + zz, 1), cols(p)], zrecv.at[p, zz])
        for d in range(1, XY):
            pcopy(p, d).start()
        return c

    def from_p(p, c=0):
        for d in range(1, XY):
            t = ppeer(d)[1]
            arrived(g.at[rows(t * Z, Z), cols(p)], precv.at[p, t])
        ccopy(p).start()
        return c

    lax.fori_loop(0, nk, send_z, 0)

    def mref(first, count):
        return meta.at[pl.ds(core * S + first, count)]

    mz = [remote(mref(xy * Z + z, 1), mzsend.at[d], mzrecv.at[z], zpeer(d)[0]) for d in range(1, Z)]
    mp = [remote(mref(xy * Z, Z), mpsend.at[d], mprecv.at[xy], ppeer(d)[0]) for d in range(1, XY)]
    mc = remote(mref(0, S), mcsend.at[0], mcrecv.at[0], partner)
    for copy in mz:
        copy.start()
    acc[...] = jnp.zeros_like(acc)

    for p in range(lead_z):
        from_z(p)
    for d in range(1, Z):
        zz = zpeer(d)[1]
        arrived(mref(xy * Z + zz, 1), mzrecv.at[zz])
    for copy in mp:
        copy.start()
    for p in range(lead_p):
        from_p(p)

    def step(k, c):
        @pl.when(k + lead_z < nk)
        def _():
            from_z(k + lead_z)

        @pl.when(k + lead_p < nk)
        def _():
            from_p(k + lead_p)

        arrived(g.at[pl.ds(pl.multiple_of((1 - core) * S * td, S * td), S * td), cols(k)], crecv.at[k])
        s = lax.rem(k, nbuf)
        wcopy(k).wait()
        acc[...] += lax.dot_general(wbuf[s], g[:, cols(k)], (((1,), (1,)), ((), ())),
                                    preferred_element_type=jnp.float32)

        @pl.when(k + nbuf < nk)
        def _():
            wcopy(k + nbuf).start(priority=1)

        return c

    lax.fori_loop(0, nk, step, 0)

    for d in range(1, XY):
        t = ppeer(d)[1]
        arrived(mref(t * Z, Z), mprecv.at[t])
    mc.start()
    arrived(meta.at[pl.ds((1 - core) * S, S)], mcrecv.at[0])

    info = jnp.sum(meta[...], axis=0)
    voc_dev = acc.shape[0]
    wanted = info[:1] - me * voc_dev
    logits = acc[...]
    top = jnp.max(logits, axis=0, keepdims=True)
    expsum = jnp.sum(jnp.exp(logits - top), axis=0, keepdims=True)
    entry = lax.broadcasted_iota(jnp.int32, logits.shape, 0)
    picked = jnp.sum(jnp.where(entry == wanted, logits, 0.0), axis=0, keepdims=True)
    mine[...] = jnp.concatenate([top + jnp.log(expsum), picked], axis=0)

    def qcopy(t, src_dev):
        return pltpu.make_async_remote_copy(
            mine, sbuf.at[src_dev], qsend.at[t], qrecv.at[src_dev],
            device_id=(t // V, lax.rem(t, V)), device_id_type=MESH)

    def qstart(d, c):
        qcopy(lax.rem(me + d, N), me).start()
        return c

    def qwait(d, c):
        t = lax.rem(me + d, N)
        qcopy(t, t).wait()
        return c

    lax.fori_loop(1, N, qstart, 0)
    sbuf[me] = mine[...]

    def drain(p, c):
        for d in range(1, Z):
            zcopy(p, d).wait_send()
        for d in range(1, XY):
            pcopy(p, d).wait_send()
        ccopy(p).wait_send()
        return c

    lax.fori_loop(0, nk, drain, 0)
    for copy in mz + mp + [mc]:
        copy.wait_send()
    lax.fori_loop(1, N, qwait, 0)

    allstat = sbuf[...]
    lse = allstat[:, 0, :]
    top = jnp.max(lse, axis=0, keepdims=True)
    total = top + jnp.log(jnp.sum(jnp.exp(lse - top), axis=0, keepdims=True))
    nll = total - jnp.sum(allstat[:, 1, :], axis=0, keepdims=True)
    row = lax.broadcasted_iota(jnp.int32, (NBENCH, tokens), 0)
    lanes = lax.broadcasted_iota(jnp.int32, (NBENCH, tokens), 1)
    hot = info[1:2] == row
    place = lax.broadcasted_iota(jnp.int32, (NBENCH, 128), 1)
    diagonal = place == lax.broadcasted_iota(jnp.int32, (NBENCH, 128), 0)

    def laid(column):
        return jnp.sum(jnp.where(diagonal, column, 0.0), axis=0, keepdims=True)

    own_nll = jnp.sum(jnp.where(lanes == at + row, nll, 0.0), axis=1, keepdims=True)
    nll_out[...] = laid(own_nll)[:, :td]
    total_out[...] = laid(jnp.sum(jnp.where(hot, nll, 0.0), axis=1, keepdims=True))[:, :NBENCH]
    count_out[...] = laid(jnp.sum(jnp.where(hot, 1.0, 0.0), axis=1, keepdims=True))[:, :NBENCH]


def solution(mesh):
    ndp, V = mesh.shape["dp"], mesh.shape["vocab"]
    N = ndp * V
    X = max(1, ndp // 2)
    Y = math.gcd(X, V)
    Z = V // Y

    def body(hidden, lm_head, targets, segment, pad_mask, seq_bench):
        td, depth = hidden.shape
        voc_dev = lm_head.shape[1]
        nseq = seq_bench.shape[0]
        tokens = N * td
        nk = 16
        kc = depth // nk
        wbytes = kc * (-(-voc_dev // 8) * 8) * 2
        held = tokens * depth * 2 + tokens * (-(-voc_dev // 128) * 128) * 4
        nbuf = max(2, min(nk, ((61 << 20) - held) // wbytes))
        lead_z, lead_p = 6, 2
        S = N // 2
        dims = (X, Y, Z, V, N, kc, nk, nbuf, td, lead_z, lead_p)
        vmem = pl.BlockSpec(memory_space=pltpu.VMEM)
        hbm = pl.BlockSpec(memory_space=pltpu.MemorySpace.HBM)
        dma = pltpu.SemaphoreType.DMA
        nll, total, count = pl.pallas_call(
            functools.partial(kernel, dims),
            out_shape=[jax.ShapeDtypeStruct((1, td), jnp.float32),
                       jax.ShapeDtypeStruct((1, NBENCH), jnp.float32),
                       jax.ShapeDtypeStruct((1, NBENCH), jnp.float32)],
            in_specs=[hbm] * 6,
            out_specs=[vmem] * 3,
            scratch_shapes=[
                pltpu.VMEM((tokens, depth), jnp.bfloat16),
                pltpu.VMEM((nbuf, voc_dev, kc), jnp.bfloat16),
                pltpu.VMEM((voc_dev, tokens), jnp.float32),
                pltpu.VMEM((N, 2, tokens), jnp.int32),
                pltpu.VMEM((1, td), jnp.int32),
                pltpu.VMEM((1, td), jnp.int32),
                pltpu.VMEM((1, td), jnp.int32),
                pltpu.VMEM((1, nseq), jnp.int32),
                pltpu.VMEM((2, tokens), jnp.float32),
                pltpu.VMEM((N, 2, tokens), jnp.float32),
                dma((nbuf,)), dma, dma((4,)),
                dma((nk, Z)), dma((nk, X * Y)), dma((nk,)),
                dma((nk, Z)), dma((nk, X * Y)), dma((nk,)),
                dma((Z,)), dma((X * Y,)), dma((1,)),
                dma((Z,)), dma((X * Y,)), dma((1,)),
                dma((N,)), dma((N,)),
            ],
            compiler_params=pltpu.CompilerParams(
                collective_id=0, has_side_effects=True, vmem_limit_bytes=67043328),
        )(hidden, targets.reshape(1, td), segment.reshape(1, td), pad_mask.reshape(1, td),
          seq_bench.reshape(1, nseq), lm_head.T)
        return nll.reshape(td), total.reshape(NBENCH), count.reshape(NBENCH)

    both = ("dp", "vocab")
    in_specs = (P(both, None), P(None, both), P(both), P(both), P(both), P())
    return jax.shard_map(body, mesh=mesh, in_specs=in_specs, out_specs=(P(both), P(), P()),
                         check_vma=False)
```
